32 devices in a mesh: mem: 8 (over y, x, core), patch: 4 (over z).
Axes of the slice: x: 2, y: 2, z: 4, core: 2. Of those that a mesh axis runs over, the one named last changes fastest.
Arguments:
- state: bfloat16 [1024, 16384], P('mem', 'patch'), may hold values from -6 to 6
- obs_ens: bfloat16 [1024, 8192], P('mem', 'patch'), may hold values from -6 to 6
- obs_values: float32 [8192], P('patch'), may hold values from -8 to 8
- obs_weight: float32 [8192], P('patch'), may hold values from 0.2 to 5
- counts: int32 [32], P('patch'), may hold values from 32 to 256
Outputs:
- analysis: bfloat16 [1024, 16384], P('mem', 'patch')
The draws below stay inside these ranges and needn't reach their ends.
Inputs may be any that keep to these rules, and one draw needn't show every extreme that they name: Region r uses the first counts[r] of its 256 observations.
All inputs are finite; a program needn't handle non-finite values. Where the reference program divides by a largest or mean magnitude, that divisor is 1e-20 or more.
Results may differ from the reference program's by a relative error of at most 0.0047.
Values may be sent and summed in bfloat16 or wider, within the bound.
A program may use at most 64 MiB of HBM per device.

```python
import math
import jax
import jax.numpy as jnp
from jax import lax

MEMBERS = 1024
REGION_ROWS = 512
OBS_OWN = 256
DEGREE = 7
REGIONS_PATCH = 8
REGIONS = 32
NROWS = 16384
NOBS = 8192


def set_ends(array, stream_key, low, high):
    longest = array.shape.index(max(array.shape))
    spots = []
    for shift in (0, 1):
        where = [jax.random.randint(jax.random.fold_in(stream_key, axis), (), 0, length) for axis, length in enumerate(array.shape)]
        where[longest] = (where[longest] + shift) % array.shape[longest]
        spots.append(tuple(where))
    return array.at[spots[0]].set(low).at[spots[1]].set(high)


def level_of(key, extent, cuts, least, top_value):
    loudness = 1.0
    for axis_at, blocks in cuts:
        heights = jax.random.uniform(jax.random.fold_in(jax.random.fold_in(key, 6), axis_at), (blocks,), jnp.float32, least / len(cuts), top_value / len(cuts))
        loudness = loudness * jnp.repeat(jnp.exp(heights), extent[axis_at] // blocks).reshape((-1,) + (1,) * (len(extent) - 1 - axis_at))
    return loudness


def bell_draw(own_key, dims, width, reach, shards=(), kind=jnp.bfloat16):
    array = jax.random.normal(own_key, dims, jnp.float32) * width
    if len(shards) > 0:
        array = level_of(own_key, dims, shards, -0.22, 0.18) * array
    return jnp.clip(array, min=-reach, max=reach).astype(kind)


def setup_inputs(seed: int = 0) -> dict:
    arg_keys = jax.random.split(jax.random.key(seed), 6)
    return {
        "state": bell_draw(arg_keys[0], (MEMBERS, NROWS), 1.0, 6.0, ((0, 8), (1, 4))),
        "obs_ens": bell_draw(arg_keys[1], (MEMBERS, NOBS), 1.0, 6.0, ((0, 8), (1, 4))),
        "obs_values": bell_draw(arg_keys[2], (NOBS,), 1.5, 8.0, ((0, 4),), jnp.float32),
        "obs_weight": jnp.clip(jnp.exp(math.log(5.0) - 3.218876 * jax.random.uniform(arg_keys[3], (NOBS,), jnp.float32) ** level_of(arg_keys[3], (NOBS,), ((0, 4),), -0.2, 0.2)), 0.2, 5.0),
        "counts": set_ends(jax.random.randint(arg_keys[4], (REGIONS,), OBS_OWN // 8, OBS_OWN + 1), jax.random.fold_in(arg_keys[4], 1), OBS_OWN // 8, OBS_OWN).astype(jnp.int32),
    }


def root_curve(values):
    lifted = jnp.sqrt(1.0 + values)
    return -1.0 / (lifted * (1.0 + lifted))

def inverse_curve(values):
    return 1.0 / (1.0 + values)

def chebyshev(upper, curve):
    number = DEGREE + 1
    theta = (jnp.arange(number, dtype=jnp.float32) + 0.5) * (math.pi / number)
    nodes = upper * (jnp.cos(theta) + 1.0) * 0.5
    samples = curve(nodes)
    orders = jnp.arange(number, dtype=jnp.float32)
    table = jnp.cos(orders[:, None] * theta[None, :])
    coefs = 2.0 / number * lax.optimization_barrier(jnp.sum(table * samples[None, :], axis=1))
    return coefs * jnp.where(orders == 0.0, 0.5, 1.0)

def clenshaw(block, matrix, coefs):
    nearer = coefs[DEGREE] * block
    farther = jnp.zeros_like(block)
    for order in range(DEGREE - 1, 0, -1):
        current = coefs[order] * block + 2.0 * jnp.dot(nearer, matrix, precision=lax.Precision.HIGHEST) - farther
        farther, nearer = (nearer, current)
    return coefs[0] * block + jnp.dot(nearer, matrix, precision=lax.Precision.HIGHEST) - farther

def perturb_obs(obs_block, values, weights, count):
    full = obs_block.astype(jnp.float32)
    centre = lax.optimization_barrier(jnp.mean(full, axis=0))
    mask = (jnp.arange(values.shape[0], dtype=jnp.int32) < count).astype(jnp.float32)
    root = jnp.sqrt(weights * mask)
    gains = ((full - centre[None, :]) * root[None, :]).astype(jnp.bfloat16)
    innov = (root * (values - centre)).astype(jnp.bfloat16)
    return jnp.concatenate([gains, innov[None, :]], axis=0)

def transform(region_state, stacked):
    gains = stacked[:-1]
    innov = stacked[-1].astype(jnp.float32)
    members = gains.shape[0]
    normal = jnp.dot(gains.T, gains, preferred_element_type=jnp.float32) / (members - 1)
    upper = jnp.max(lax.optimization_barrier(jnp.sum(jnp.abs(normal), axis=1))) + 1e-06
    shifted = normal * (2.0 / upper) - jnp.eye(normal.shape[0], dtype=jnp.float32)
    full = region_state.astype(jnp.float32)
    centre = lax.optimization_barrier(jnp.mean(full, axis=0))
    spread = (full - centre[None, :]).astype(jnp.bfloat16)
    product = jnp.dot(spread.T, gains, preferred_element_type=jnp.float32)
    mixed = clenshaw(product, shifted, chebyshev(upper, root_curve)).astype(jnp.bfloat16)
    mean_weights = clenshaw(innov[None, :], shifted, chebyshev(upper, inverse_curve))[0]
    mean_shift = jnp.dot(product, mean_weights, precision=lax.Precision.HIGHEST) / (members - 1)
    update = jnp.dot(gains, mixed.T, preferred_element_type=jnp.float32) / (members - 1)
    return (full + mean_shift[None, :] + update).astype(jnp.bfloat16)

def reference(state, obs_ens, obs_values, obs_weight, counts):
    order = jnp.arange(REGIONS, dtype=jnp.int32)

    def own_part(region):
        start = region * OBS_OWN
        block = lax.dynamic_slice_in_dim(obs_ens, start, OBS_OWN, 1)
        values = lax.dynamic_slice_in_dim(obs_values, start, OBS_OWN, 0)
        weights = lax.dynamic_slice_in_dim(obs_weight, start, OBS_OWN, 0)
        return perturb_obs(block, values, weights, counts[region])
    stacked = lax.map(own_part, order)
    half = OBS_OWN // 2

    def one_region(region):
        left = stacked[(region - REGIONS_PATCH) % REGIONS][:, OBS_OWN - half:]
        right = stacked[(region + REGIONS_PATCH) % REGIONS][:, :half]
        joined = jnp.concatenate([left, stacked[region], right], axis=1)
        block = lax.dynamic_slice_in_dim(state, region * REGION_ROWS, REGION_ROWS, 1)
        return transform(block, joined)
    result = lax.map(one_region, order)
    return jnp.transpose(result, (1, 0, 2)).reshape(MEMBERS, NROWS)
```

```python
import functools
import math

import jax
import jax.numpy as jnp
import numpy as np
from jax import lax
from jax.experimental import pallas as pl
from jax.experimental.pallas import tpu as pltpu
from jax.sharding import PartitionSpec as P

DEGREE = 7
MESH = pl.DeviceIdType.MESH
PAD = 16
CHUNKS = 2


def functionals():
    number = DEGREE + 1
    theta = (np.arange(number) + 0.5) * (math.pi / number)
    rows = 2.0 / number * np.cos(np.arange(number)[:, None] * theta[None, :])
    rows[0] *= 0.5
    a = rows
    signs = np.where(np.arange(number) % 2 == 0, 1.0, -1.0)
    table = np.stack(
        [
            (signs[:, None] * a).sum(0),
            a[1] - a[7] + 2 * a[5],
            a[2] + a[6],
            a[3] - a[5] + 2 * a[7],
            a[4] - 2 * a[5] + 2 * a[6] - 2 * a[7],
            2 * a[5],
            2 * a[6],
            2 * a[7],
        ]
    )
    return (np.cos(theta) + 1.0) * 0.5, table


def flipped(index, step, count):
    bit = 1
    while bit < count:
        if step & bit:
            index = index + bit - 2 * bit * (lax.rem(index // bit, 2))
        bit *= 2
    return index


def dot(left, right):
    return jnp.dot(left, right, preferred_element_type=jnp.float32)


def pair_rows(row):
    high = row.astype(jnp.bfloat16).astype(jnp.float32)
    k = row.shape[1]
    pick = lax.broadcasted_iota(jnp.int32, (PAD, k), 0)
    wide = (PAD, k)
    return jnp.where(
        pick == 0,
        jnp.broadcast_to(high, wide),
        jnp.where(pick == 1, jnp.broadcast_to(row - high, wide), 0.0),
    ).astype(jnp.bfloat16)


def rows_sum(block):
    return jnp.sum(block, axis=0, keepdims=True)


def kernel(
    n, npatch,
    val_hbm, wgt_hbm, cnt_hbm, obs_hbm, state_hbm, out_hbm,
    val_v, wgt_v, cnt_s, side, obs_s, state_s, edge_v, obs_v, state_v, gain, gain_t, acc, pt, out_v,
    d1, d2, d4, px, mix,
    obs_ss, obs_rs, st_ss, st_rs, edge_ss, edge_rs, side_ss, side_rs, out_ss, out_rs, loc,
):
    me = lax.axis_index("mem")
    patch = lax.axis_index("patch")
    rows = obs_hbm.shape[0]
    own = obs_v.shape[1]
    half = own // 2
    width = state_v.shape[1]
    wc = width // CHUNKS
    members = n * rows
    nobs = 2 * own
    up = lax.rem(patch + 1, npatch)
    down = lax.rem(patch + npatch - 1, npatch)
    f32, bf = jnp.float32, jnp.bfloat16

    def cols(index, size):
        return pl.ds(pl.multiple_of(index * size, size), size)

    def part(index, c):
        return pl.ds(pl.multiple_of(index * width + c * wc, wc), wc)

    group = max(1, 256 // rows)
    groups = n // group
    gr = group * rows
    far = list(range(1, groups))
    near = list(range(1, group))
    steps = near + [s * group + i for i in range(group) for s in far]
    order = [0] + far

    barrier = pltpu.get_barrier_semaphore()
    for s in steps:
        pl.semaphore_signal(barrier, inc=1, device_id=(flipped(me, s, n), patch), device_id_type=MESH)
    for p in (up, down):
        pl.semaphore_signal(barrier, inc=1, device_id=(me, p), device_id_type=MESH)
    load_obs = pltpu.make_async_copy(obs_hbm, obs_s, loc.at[6])
    load_obs.start()
    own_obs = pltpu.make_async_copy(obs_hbm.at[:, cols(me, own)], obs_v.at[cols(me, rows), :], loc.at[0])
    own_obs.start()
    small = [
        pltpu.make_async_copy(src, dst, loc.at[3 + i])
        for i, (src, dst) in enumerate(((val_hbm, val_v), (wgt_hbm, wgt_v), (cnt_hbm, cnt_s)))
    ]
    for c in small:
        c.start()
    load_state = pltpu.make_async_copy(state_hbm, state_s, loc.at[7])
    load_state.start()
    own_state = pltpu.make_async_copy(state_hbm.at[:, cols(me, width)], state_v.at[cols(me, rows), :], loc.at[1])
    own_state.start()

    def obs_copy(s):
        peer = flipped(me, s, n)
        return pltpu.make_async_remote_copy(
            src_ref=obs_s.at[:, cols(peer, own)], dst_ref=obs_v.at[cols(me, rows), :],
            send_sem=obs_ss.at[s], recv_sem=obs_rs.at[s], device_id=(peer, patch), device_id_type=MESH)

    def state_copy(s, c):
        peer = flipped(me, s, n)
        return pltpu.make_async_remote_copy(
            src_ref=state_s.at[:, part(peer, c)], dst_ref=state_v.at[cols(me, rows), pl.ds(c * wc, wc)],
            send_sem=st_ss.at[c, s], recv_sem=st_rs.at[c, s], device_id=(peer, patch), device_id_type=MESH)

    def out_copy(s, c):
        peer = flipped(me, s, n)
        return pltpu.make_async_remote_copy(
            src_ref=out_v.at[cols(peer, rows), pl.ds(c * wc, wc)], dst_ref=out_hbm.at[:, part(me, c)],
            send_sem=out_ss.at[c, s], recv_sem=out_rs.at[c, s], device_id=(peer, patch), device_id_type=MESH)

    def edge_copy(slot, s):
        block = cols(flipped(me, s, n), rows)
        return pltpu.make_async_remote_copy(
            src_ref=obs_v.at[block, pl.ds((1 - slot) * half, half)], dst_ref=edge_v.at[slot, block, :],
            send_sem=edge_ss.at[slot, s], recv_sem=edge_rs.at[slot, s],
            device_id=(me, down if slot else up), device_id_type=MESH)

    def side_copy(slot):
        return pltpu.make_async_remote_copy(
            src_ref=side.at[1 - slot], dst_ref=side.at[2 + slot],
            send_sem=side_ss.at[slot], recv_sem=side_rs.at[slot],
            device_id=(me, down if slot else up), device_id_type=MESH)

    load_obs.wait()
    own_obs.wait()
    pl.semaphore_wait(barrier, n + 1)
    for s in near:
        obs_copy(s).start()
    for slot in range(2):
        edge_copy(slot, 0).start()
    for s in steps:
        if s >= group:
            obs_copy(s).start()
    load_state.wait()
    for c in range(CHUNKS):
        for s in steps:
            state_copy(s, c).start()

    for c in small:
        c.wait()
    count = cnt_s[me]
    roots = []
    for k in range(2):
        lane = lax.broadcasted_iota(jnp.int32, (1, half), 1) + k * half
        mask = jnp.where(lane < count, 1.0, 0.0)
        roots.append(jnp.sqrt(wgt_v[pl.ds(2 * me + k, 1), :] * mask))

    for s in steps:
        obs_copy(s).wait_recv()
        for slot in range(2):
            edge_copy(slot, s).start()

    def perturb(k, block, at, centre, root):
        scaled_block = ((block.astype(f32) - centre) * root).astype(bf)
        gain[k, at, :] = scaled_block
        gain_t[pl.ds(k * half, half), at] = scaled_block.T

    innovs = [None] * 4

    def innov(k, centre, root, values):
        innovs[k] = (root * (values - centre)).astype(bf).astype(f32)

    for k in range(2):
        block = obs_v[:, k * half:(k + 1) * half]
        centre = rows_sum(block.astype(f32)) * (1.0 / members)
        values = val_v[pl.ds(2 * me + k, 1), :]
        pick = lax.broadcasted_iota(jnp.int32, (8, half), 0)
        side[k] = jnp.where(pick == 0, roots[k], jnp.where(pick == 1, values, centre))
        innov(k, centre, roots[k], values)
        perturb(k, block, pl.ds(0, members), centre, roots[k])
    for slot in range(2):
        side_copy(slot).start()
    for slot in range(2):
        side_copy(slot).wait_recv()
    edge_root, edge_centre = [], []
    for slot in range(2):
        root, values, centre = (side[2 + slot, pl.ds(i, 1), :] for i in range(3))
        edge_root.append(root)
        edge_centre.append(centre)
        innov(2 + slot, centre, root, values)
    dvec = jnp.concatenate(innovs, axis=1)

    def gains_of(at):
        return jnp.concatenate([gain[k, at, :] for k in range(4)], axis=1)

    normal = None
    for i, s in enumerate(order):
        base = flipped(me // group, s, groups)
        at = cols(base, gr)
        for slot in range(2):
            for j in range(group):
                edge_copy(slot, s * group + j).wait_recv()
        for slot in range(2):
            perturb(2 + slot, edge_v[slot, at, :], at, edge_centre[slot], edge_root[slot])
        piece = dot(gain_t[:, at], gains_of(at))
        if i < groups - 1:
            acc[...] = piece if i == 0 else acc[...] + piece
        else:
            normal = piece if i == 0 else acc[...] + piece

    upper = jnp.max(jnp.sum(jnp.abs(normal), axis=0, keepdims=True), axis=1, keepdims=True)
    upper = upper * (1.0 / (members - 1)) + 1e-06
    t = normal * (2.0 / (members - 1) / upper)
    d1[pl.ds(0, nobs), :] = t.astype(bf)
    d1[pl.ds(nobs, PAD), :] = pair_rows(dvec)

    nodes, table = functionals()
    wide = jnp.broadcast_to(upper, (1, nobs))
    f_samples, e_samples = [], []
    for k in range(DEGREE + 1):
        m = wide * float(nodes[k])
        lifted = jnp.sqrt(1.0 + m)
        f_samples.append(-1.0 / (lifted * (1.0 + lifted)))
        e_samples.append(1.0 / (1.0 + m))

    def combined(samples):
        out = []
        for j in range(DEGREE + 1):
            total = samples[0] * float(table[j, 0])
            for k in range(1, DEGREE + 1):
                total = total + samples[k] * float(table[j, k])
            out.append(total)
        return out

    fa = combined(f_samples)
    ea = combined(e_samples)
    top, extra = pl.ds(0, nobs), pl.ds(nobs, PAD)

    r1 = d1[top, :]
    prod = dot(d1[...], r1)
    second = 2.0 * prod[:nobs] - 4.0 * t
    y1 = rows_sum(prod[nobs:])
    d2[top, :] = second.astype(bf)
    d2[extra, :] = pair_rows(y1)
    r2 = d2[top, :]
    prod3 = dot(d1[...], r2)
    prod4 = dot(d2[...], r2)
    third = 2.0 * prod3[:nobs] + t - 2.0 * second
    fourth = 2.0 * prod4[:nobs] + 4.0 * second
    d4[...] = fourth.astype(bf)
    y2 = rows_sum(prod3[nobs:])
    y3 = 2.0 * rows_sum(prod4[nobs:]) + y1 - 2.0 * y2
    px[top, :] = (fa[5] * t + fa[6] * second + fa[7] * third).astype(bf)
    px[extra, :] = pair_rows(ea[5] * y1 + ea[6] * y2 + ea[7] * y3 + ea[4] * dvec)
    low = fa[1] * t + fa[2] * second + fa[3] * third + fa[4] * fourth
    prod7 = dot(px[...], d4[...])
    poly = low + prod7[:nobs]
    u = ea[0] * dvec + ea[1] * y1 + ea[2] * y2 + ea[3] * y3 + rows_sum(prod7[nobs:])
    px[top, :] = poly.astype(bf)
    px[extra, :] = pair_rows(u)

    gsum = jnp.sum(gain_t[...].astype(f32), axis=1, keepdims=True)
    scale = 1.0 / (members - 1)
    fa0 = fa[0][:, 0:1]

    for c in range(CHUNKS):
        here = pl.ds(c * wc, wc)
        csum = jnp.zeros((1, wc), f32)
        if c == 0:
            own_state.wait()
        for i, s in enumerate(order):
            base = flipped(me // group, s, groups)
            for j in range(group):
                if s * group + j:
                    state_copy(s * group + j, c).wait_recv()
            block = state_v[cols(base, gr), here]
            csum = csum + rows_sum(block.astype(f32))
            piece = dot(gain_t[:, cols(base, gr)], block)
            pt[...] = piece if i == 0 else pt[...] + piece
        product = pt[...] - gsum * (csum * (1.0 / members))
        product_b = product.astype(bf)
        both = dot(px[...], product_b)
        mix[...] = ((fa0 * product + both[:nobs]) * scale).astype(bf)
        shift = rows_sum(both[nobs:]) * scale
        for s in far + [0]:
            base = flipped(me // group, s, groups)
            at = cols(base, gr)
            update = dot(gains_of(at), mix[...])
            out_v[at, here] = (state_v[at, here].astype(f32) + shift + update).astype(bf)
            for j in range(group):
                if s * group + j:
                    out_copy(s * group + j, c).start()
    keep = pltpu.make_async_copy(out_v.at[cols(me, rows), :], out_hbm.at[:, cols(me, width)], loc.at[2])
    keep.start()

    for slot in range(2):
        side_copy(slot).wait_send()
        for s in range(n):
            edge_copy(slot, s).wait_send()
    for s in steps:
        obs_copy(s).wait_send()
        for c in range(CHUNKS):
            state_copy(s, c).wait_send()
    keep.wait()
    for c in range(CHUNKS):
        for s in steps:
            out_copy(s, c).wait()


def on_device(n, npatch, state, obs_ens, obs_values, obs_weight, counts):
    rows = obs_ens.shape[0]
    own = obs_ens.shape[1] // n
    width = state.shape[1] // n
    members = rows * n
    nobs = 2 * own
    half = own // 2
    wc = width // CHUNKS
    bf, f32 = jnp.bfloat16, jnp.float32
    dma = pltpu.SemaphoreType.DMA
    hbm = pl.BlockSpec(memory_space=pl.ANY)
    return pl.pallas_call(
        functools.partial(kernel, n, npatch),
        out_shape=jax.ShapeDtypeStruct(state.shape, bf),
        in_specs=[pl.BlockSpec(memory_space=pltpu.HBM)] * 5,
        out_specs=hbm,
        scratch_shapes=[
            pltpu.VMEM((2 * n, half), f32),
            pltpu.VMEM((2 * n, half), f32),
            pltpu.SMEM((n,), jnp.int32),
            pltpu.VMEM((4, 8, half), f32),
            pltpu.VMEM(obs_ens.shape, bf),
            pltpu.VMEM(state.shape, bf),
            pltpu.VMEM((2, members, half), bf),
            pltpu.VMEM((members, own), bf),
            pltpu.VMEM((members, width), bf),
            pltpu.VMEM((4, members, half), bf),
            pltpu.VMEM((nobs, members), bf),
            pltpu.VMEM((nobs, nobs), f32),
            pltpu.VMEM((nobs, wc), f32),
            pltpu.VMEM((members, width), bf),
            pltpu.VMEM((nobs + PAD, nobs), bf),
            pltpu.VMEM((nobs + PAD, nobs), bf),
            pltpu.VMEM((nobs, nobs), bf),
            pltpu.VMEM((nobs + PAD, nobs), bf),
            pltpu.VMEM((nobs, wc), bf),
            dma((n,)), dma((n,)), dma((CHUNKS, n)), dma((CHUNKS, n)),
            dma((2, n)), dma((2, n)), dma((2,)), dma((2,)), dma((CHUNKS, n)), dma((CHUNKS, n)), dma((8,)),
        ],
        compiler_params=pltpu.CompilerParams(collective_id=0, has_side_effects=True, vmem_limit_bytes=28 * 1024 * 1024),
    )(*(pltpu.with_memory_space_constraint(x, pltpu.HBM) for x in (obs_values.reshape(2 * n, half), obs_weight.reshape(2 * n, half), counts, obs_ens, state)))


def solution(mesh):
    placed = (P("mem", "patch"), P("mem", "patch"), P("patch"), P("patch"), P("patch"))
    body = functools.partial(on_device, mesh.shape["mem"], mesh.shape["patch"])
    return jax.shard_map(
        body, mesh=mesh, in_specs=placed, out_specs=P("mem", "patch"), check_vma=False
    )
```

```python
import functools
import math

import jax
import jax.numpy as jnp
import numpy as np
from jax import lax
from jax.experimental import pallas as pl
from jax.experimental.pallas import tpu as pltpu
from jax.sharding import PartitionSpec as P

DEGREE = 7
MESH = pl.DeviceIdType.MESH
PAD = 16
CHUNKS = 2


def functionals():
    number = DEGREE + 1
    theta = (np.arange(number) + 0.5) * (math.pi / number)
    rows = 2.0 / number * np.cos(np.arange(number)[:, None] * theta[None, :])
    rows[0] *= 0.5
    a = rows
    signs = np.where(np.arange(number) % 2 == 0, 1.0, -1.0)
    table = np.stack(
        [
            (signs[:, None] * a).sum(0),
            a[1] - a[7] + 2 * a[5],
            a[2] + a[6],
            a[3] - a[5] + 2 * a[7],
            a[4] - 2 * a[5] + 2 * a[6] - 2 * a[7],
            2 * a[5],
            2 * a[6],
            2 * a[7],
        ]
    )
    return (np.cos(theta) + 1.0) * 0.5, table


def flipped(index, step, count):
    bit = 1
    while bit < count:
        if step & bit:
            index = index + bit - 2 * bit * (lax.rem(index // bit, 2))
        bit *= 2
    return index


def dot(left, right):
    return jnp.dot(left, right, preferred_element_type=jnp.float32)


def pair_rows(row):
    high = row.astype(jnp.bfloat16).astype(jnp.float32)
    k = row.shape[1]
    pick = lax.broadcasted_iota(jnp.int32, (PAD, k), 0)
    wide = (PAD, k)
    return jnp.where(
        pick == 0,
        jnp.broadcast_to(high, wide),
        jnp.where(pick == 1, jnp.broadcast_to(row - high, wide), 0.0),
    ).astype(jnp.bfloat16)


def rows_sum(block):
    return jnp.sum(block, axis=0, keepdims=True)


def kernel(
    n, npatch,
    val_hbm, wgt_hbm, cnt_hbm, obs_hbm, state_hbm, out_hbm,
    val_v, wgt_v, cnt_s, side, obs_s, state_s, edge_v, obs_v, state_v, gain, gain_t, acc, pt, out_v,
    d1, d2, d4, px, mix,
    obs_ss, obs_rs, st_ss, st_rs, edge_ss, edge_rs, side_ss, side_rs, out_ss, out_rs, loc,
):
    me = lax.axis_index("mem")
    patch = lax.axis_index("patch")
    rows = obs_hbm.shape[0]
    own = obs_v.shape[1]
    half = own // 2
    width = state_v.shape[1]
    wc = width // CHUNKS
    members = n * rows
    nobs = 2 * own
    up = lax.rem(patch + 1, npatch)
    down = lax.rem(patch + npatch - 1, npatch)
    f32, bf = jnp.float32, jnp.bfloat16

    def cols(index, size):
        return pl.ds(pl.multiple_of(index * size, size), size)

    def part(index, c):
        return pl.ds(pl.multiple_of(index * width + c * wc, wc), wc)

    group = max(1, 256 // rows)
    groups = n // group
    gr = group * rows
    far = list(range(1, groups))
    mine = me // group
    near = list(range(1, group))
    steps = near + [s * group + i for i in range(group) for s in far]
    order = [0] + far

    barrier = pltpu.get_barrier_semaphore()
    for s in steps:
        pl.semaphore_signal(barrier, inc=1, device_id=(flipped(me, s, n), patch), device_id_type=MESH)
    for p in (up, down):
        pl.semaphore_signal(barrier, inc=1, device_id=(me, p), device_id_type=MESH)
    load_obs = pltpu.make_async_copy(obs_hbm, obs_s, loc.at[6])
    load_obs.start()
    own_obs = pltpu.make_async_copy(obs_hbm.at[:, cols(me, own)], obs_v.at[cols(me, rows), :], loc.at[0])
    own_obs.start()
    small = [
        pltpu.make_async_copy(src, dst, loc.at[3 + i])
        for i, (src, dst) in enumerate(((val_hbm, val_v), (wgt_hbm, wgt_v), (cnt_hbm, cnt_s)))
    ]
    for c in small:
        c.start()
    load_state = pltpu.make_async_copy(state_hbm, state_s, loc.at[7])
    load_state.start()
    own_state = pltpu.make_async_copy(state_hbm.at[:, cols(me, width)], state_v.at[cols(me, rows), :], loc.at[1])
    own_state.start()

    def obs_copy(s):
        peer = flipped(me, s, n)
        return pltpu.make_async_remote_copy(
            src_ref=obs_s.at[:, cols(peer, own)], dst_ref=obs_v.at[cols(me, rows), :],
            send_sem=obs_ss.at[s], recv_sem=obs_rs.at[s], device_id=(peer, patch), device_id_type=MESH)

    def state_copy(s, c):
        peer = flipped(me, s, n)
        return pltpu.make_async_remote_copy(
            src_ref=state_s.at[:, part(peer, c)], dst_ref=state_v.at[cols(me, rows), pl.ds(c * wc, wc)],
            send_sem=st_ss.at[c, s], recv_sem=st_rs.at[c, s], device_id=(peer, patch), device_id_type=MESH)

    def out_copy(s, c):
        peer = flipped(me, s, n)
        return pltpu.make_async_remote_copy(
            src_ref=out_v.at[cols(peer, rows), pl.ds(c * wc, wc)], dst_ref=out_hbm.at[:, part(me, c)],
            send_sem=out_ss.at[c, s], recv_sem=out_rs.at[c, s], device_id=(peer, patch), device_id_type=MESH)

    def edge_copy(slot, s):
        block = cols(flipped(me, s, n), rows)
        return pltpu.make_async_remote_copy(
            src_ref=obs_v.at[block, pl.ds((1 - slot) * half, half)], dst_ref=edge_v.at[slot, block, :],
            send_sem=edge_ss.at[slot, s], recv_sem=edge_rs.at[slot, s],
            device_id=(me, down if slot else up), device_id_type=MESH)

    def side_copy(slot):
        return pltpu.make_async_remote_copy(
            src_ref=side.at[1 - slot], dst_ref=side.at[2 + slot],
            send_sem=side_ss.at[slot], recv_sem=side_rs.at[slot],
            device_id=(me, down if slot else up), device_id_type=MESH)

    load_obs.wait()
    own_obs.wait()
    pl.semaphore_wait(barrier, n + 1)
    for s in near:
        obs_copy(s).start()
    for slot in range(2):
        edge_copy(slot, 0).start()
    for s in steps:
        if s >= group:
            obs_copy(s).start()
    load_state.wait()
    for c in range(CHUNKS):
        for s in steps:
            state_copy(s, c).start()

    for c in small:
        c.wait()
    count = cnt_s[me]
    roots = []
    for k in range(2):
        lane = lax.broadcasted_iota(jnp.int32, (1, half), 1) + k * half
        mask = jnp.where(lane < count, 1.0, 0.0)
        roots.append(jnp.sqrt(wgt_v[pl.ds(2 * me + k, 1), :] * mask))

    for s in steps:
        obs_copy(s).wait_recv()
        for slot in range(2):
            edge_copy(slot, s).start()

    def perturb(k, block, at, centre, root):
        scaled_block = ((block.astype(f32) - centre) * root).astype(bf)
        gain[k, at, :] = scaled_block
        gain_t[pl.ds(k * half, half), at] = scaled_block.T

    innovs = [None] * 4

    def innov(k, centre, root, values):
        innovs[k] = (root * (values - centre)).astype(bf).astype(f32)

    for k in range(2):
        block = obs_v[:, k * half:(k + 1) * half]
        centre = rows_sum(block.astype(f32)) * (1.0 / members)
        values = val_v[pl.ds(2 * me + k, 1), :]
        pick = lax.broadcasted_iota(jnp.int32, (8, half), 0)
        side[k] = jnp.where(pick == 0, roots[k], jnp.where(pick == 1, values, centre))
        innov(k, centre, roots[k], values)
        perturb(k, block, pl.ds(0, members), centre, roots[k])
    for slot in range(2):
        side_copy(slot).start()
    for slot in range(2):
        side_copy(slot).wait_recv()
    edge_root, edge_centre = [], []
    for slot in range(2):
        root, values, centre = (side[2 + slot, pl.ds(i, 1), :] for i in range(3))
        edge_root.append(root)
        edge_centre.append(centre)
        innov(2 + slot, centre, root, values)
    dvec = jnp.concatenate(innovs, axis=1)

    def gains_of(at):
        return jnp.concatenate([gain[k, at, :] for k in range(4)], axis=1)

    def add_group(c, i, total):
        at = cols(flipped(mine, order[i], groups), gr)
        block = state_v[at, pl.ds(c * wc, wc)]
        piece = dot(gain_t[:, at], block)
        pt[...] = piece if i == 0 else pt[...] + piece
        return total + rows_sum(block.astype(f32))

    def state_waits(c):
        if c == 0:
            own_state.wait()
        for s in steps:
            state_copy(s, c).wait_recv()

    normal = None
    for i, s in enumerate(order):
        base = flipped(me // group, s, groups)
        at = cols(base, gr)
        for slot in range(2):
            for j in range(group):
                edge_copy(slot, s * group + j).wait_recv()
        for slot in range(2):
            perturb(2 + slot, edge_v[slot, at, :], at, edge_centre[slot], edge_root[slot])
        piece = dot(gain_t[:, at], gains_of(at))
        if i < groups - 1:
            acc[...] = piece if i == 0 else acc[...] + piece
        else:
            normal = piece if i == 0 else acc[...] + piece

    csum = jnp.zeros((1, wc), f32)
    state_waits(0)
    upper = jnp.max(jnp.sum(jnp.abs(normal), axis=0, keepdims=True), axis=1, keepdims=True)
    upper = upper * (1.0 / (members - 1)) + 1e-06
    t = normal * (2.0 / (members - 1) / upper)
    d1[pl.ds(0, nobs), :] = t.astype(bf)
    d1[pl.ds(nobs, PAD), :] = pair_rows(dvec)

    for i in range(groups):
        csum = add_group(0, i, csum)
    nodes, table = functionals()
    wide = jnp.broadcast_to(upper, (1, nobs))
    f_samples, e_samples = [], []
    for k in range(DEGREE + 1):
        m = wide * float(nodes[k])
        lifted = jnp.sqrt(1.0 + m)
        f_samples.append(-1.0 / (lifted * (1.0 + lifted)))
        e_samples.append(1.0 / (1.0 + m))

    def combined(samples):
        out = []
        for j in range(DEGREE + 1):
            total = samples[0] * float(table[j, 0])
            for k in range(1, DEGREE + 1):
                total = total + samples[k] * float(table[j, k])
            out.append(total)
        return out

    fa = combined(f_samples)
    ea = combined(e_samples)
    top, extra = pl.ds(0, nobs), pl.ds(nobs, PAD)

    r1 = d1[top, :]
    prod = dot(d1[...], r1)
    second = 2.0 * prod[:nobs] - 4.0 * t
    y1 = rows_sum(prod[nobs:])
    d2[top, :] = second.astype(bf)
    d2[extra, :] = pair_rows(y1)
    r2 = d2[top, :]
    prod3 = dot(d1[...], r2)
    prod4 = dot(d2[...], r2)
    third = 2.0 * prod3[:nobs] + t - 2.0 * second
    fourth = 2.0 * prod4[:nobs] + 4.0 * second
    d4[...] = fourth.astype(bf)
    y2 = rows_sum(prod3[nobs:])
    y3 = 2.0 * rows_sum(prod4[nobs:]) + y1 - 2.0 * y2
    px[top, :] = (fa[5] * t + fa[6] * second + fa[7] * third).astype(bf)
    px[extra, :] = pair_rows(ea[5] * y1 + ea[6] * y2 + ea[7] * y3 + ea[4] * dvec)
    low = fa[1] * t + fa[2] * second + fa[3] * third + fa[4] * fourth
    prod7 = dot(px[...], d4[...])
    poly = low + prod7[:nobs]
    u = ea[0] * dvec + ea[1] * y1 + ea[2] * y2 + ea[3] * y3 + rows_sum(prod7[nobs:])
    px[top, :] = poly.astype(bf)
    px[extra, :] = pair_rows(u)

    gsum = jnp.sum(gain_t[...].astype(f32), axis=1, keepdims=True)
    scale = 1.0 / (members - 1)
    fa0 = fa[0][:, 0:1]

    for c in range(CHUNKS):
        here = pl.ds(c * wc, wc)
        if c:
            csum = jnp.zeros((1, wc), f32)
            state_waits(c)
            for i in range(groups):
                csum = add_group(c, i, csum)
        product = pt[...] - gsum * (csum * (1.0 / members))
        product_b = product.astype(bf)
        both = dot(px[...], product_b)
        mix[...] = ((fa0 * product + both[:nobs]) * scale).astype(bf)
        shift = rows_sum(both[nobs:]) * scale
        for s in far + [0]:
            base = flipped(me // group, s, groups)
            at = cols(base, gr)
            update = dot(gains_of(at), mix[...])
            out_v[at, here] = (state_v[at, here].astype(f32) + shift + update).astype(bf)
            for j in range(group):
                if s * group + j:
                    out_copy(s * group + j, c).start()
    keep = pltpu.make_async_copy(out_v.at[cols(me, rows), :], out_hbm.at[:, cols(me, width)], loc.at[2])
    keep.start()

    for slot in range(2):
        side_copy(slot).wait_send()
        for s in range(n):
            edge_copy(slot, s).wait_send()
    for s in steps:
        obs_copy(s).wait_send()
        for c in range(CHUNKS):
            state_copy(s, c).wait_send()
    keep.wait()
    for c in range(CHUNKS):
        for s in steps:
            out_copy(s, c).wait()


def on_device(n, npatch, state, obs_ens, obs_values, obs_weight, counts):
    rows = obs_ens.shape[0]
    own = obs_ens.shape[1] // n
    width = state.shape[1] // n
    members = rows * n
    nobs = 2 * own
    half = own // 2
    wc = width // CHUNKS
    bf, f32 = jnp.bfloat16, jnp.float32
    dma = pltpu.SemaphoreType.DMA
    hbm = pl.BlockSpec(memory_space=pl.ANY)
    return pl.pallas_call(
        functools.partial(kernel, n, npatch),
        out_shape=jax.ShapeDtypeStruct(state.shape, bf),
        in_specs=[pl.BlockSpec(memory_space=pltpu.HBM)] * 5,
        out_specs=hbm,
        scratch_shapes=[
            pltpu.VMEM((2 * n, half), f32),
            pltpu.VMEM((2 * n, half), f32),
            pltpu.SMEM((n,), jnp.int32),
            pltpu.VMEM((4, 8, half), f32),
            pltpu.VMEM(obs_ens.shape, bf),
            pltpu.VMEM(state.shape, bf),
            pltpu.VMEM((2, members, half), bf),
            pltpu.VMEM((members, own), bf),
            pltpu.VMEM((members, width), bf),
            pltpu.VMEM((4, members, half), bf),
            pltpu.VMEM((nobs, members), bf),
            pltpu.VMEM((nobs, nobs), f32),
            pltpu.VMEM((nobs, wc), f32),
            pltpu.VMEM((members, width), bf),
            pltpu.VMEM((nobs + PAD, nobs), bf),
            pltpu.VMEM((nobs + PAD, nobs), bf),
            pltpu.VMEM((nobs, nobs), bf),
            pltpu.VMEM((nobs + PAD, nobs), bf),
            pltpu.VMEM((nobs, wc), bf),
            dma((n,)), dma((n,)), dma((CHUNKS, n)), dma((CHUNKS, n)),
            dma((2, n)), dma((2, n)), dma((2,)), dma((2,)), dma((CHUNKS, n)), dma((CHUNKS, n)), dma((8,)),
        ],
        compiler_params=pltpu.CompilerParams(collective_id=0, has_side_effects=True, vmem_limit_bytes=28 * 1024 * 1024),
    )(*(pltpu.with_memory_space_constraint(x, pltpu.HBM) for x in (obs_values.reshape(2 * n, half), obs_weight.reshape(2 * n, half), counts, obs_ens, state)))


def solution(mesh):
    placed = (P("mem", "patch"), P("mem", "patch"), P("patch"), P("patch"), P("patch"))
    body = functools.partial(on_device, mesh.shape["mem"], mesh.shape["patch"])
    return jax.shard_map(
        body, mesh=mesh, in_specs=placed, out_specs=P("mem", "patch"), check_vma=False
    )
```

```python
import functools
import math

import jax
import jax.numpy as jnp
import numpy as np
from jax import lax
from jax.experimental import pallas as pl
from jax.experimental.pallas import tpu as pltpu
from jax.sharding import PartitionSpec as P

DEGREE = 7
MESH = pl.DeviceIdType.MESH
PAD = 16
CHUNKS = 2


def functionals():
    number = DEGREE + 1
    theta = (np.arange(number) + 0.5) * (math.pi / number)
    rows = 2.0 / number * np.cos(np.arange(number)[:, None] * theta[None, :])
    rows[0] *= 0.5
    a = rows
    signs = np.where(np.arange(number) % 2 == 0, 1.0, -1.0)
    table = np.stack(
        [
            (signs[:, None] * a).sum(0),
            a[1] - a[7] + 2 * a[5],
            a[2] + a[6],
            a[3] - a[5] + 2 * a[7],
            a[4] - 2 * a[5] + 2 * a[6] - 2 * a[7],
            2 * a[5],
            2 * a[6],
            2 * a[7],
        ]
    )
    return (np.cos(theta) + 1.0) * 0.5, table


def flipped(index, step, count):
    bit = 1
    while bit < count:
        if step & bit:
            index = index + bit - 2 * bit * (lax.rem(index // bit, 2))
        bit *= 2
    return index


def dot(left, right):
    return jnp.dot(left, right, preferred_element_type=jnp.float32)


def pair_rows(row, third=None):
    high = row.astype(jnp.bfloat16).astype(jnp.float32)
    k = row.shape[1]
    pick = lax.broadcasted_iota(jnp.int32, (PAD, k), 0)
    wide = (PAD, k)
    return jnp.where(
        pick == 0,
        jnp.broadcast_to(high, wide),
        jnp.where(
            pick == 1,
            jnp.broadcast_to(row - high, wide),
            0.0 if third is None else jnp.where(pick == 2, jnp.broadcast_to(third, wide), 0.0),
        ),
    ).astype(jnp.bfloat16)


def rows_sum(block):
    return jnp.sum(block, axis=0, keepdims=True)


def kernel(
    n, npatch,
    val_hbm, wgt_hbm, cnt_hbm, obs_hbm, state_hbm, out_hbm,
    val_v, wgt_v, cnt_s, side, obs_s, state_s, edge_v, obs_v, state_v, gain, gain_t, acc, out_v,
    d1, d2, d4, mix,
    obs_ss, obs_rs, st_ss, st_rs, edge_ss, edge_rs, side_ss, side_rs, out_ss, out_rs, loc,
):
    me = lax.axis_index("mem")
    patch = lax.axis_index("patch")
    rows = obs_hbm.shape[0]
    own = obs_v.shape[1]
    half = own // 2
    width = state_v.shape[1]
    wc = width // CHUNKS
    members = n * rows
    nobs = 2 * own
    up = lax.rem(patch + 1, npatch)
    down = lax.rem(patch + npatch - 1, npatch)
    f32, bf = jnp.float32, jnp.bfloat16

    def cols(index, size):
        return pl.ds(pl.multiple_of(index * size, size), size)

    def part(index, c):
        return pl.ds(pl.multiple_of(index * width + c * wc, wc), wc)

    group = max(1, 256 // rows)
    groups = n // group
    gr = group * rows
    far = list(range(1, groups))
    mine = me // group
    near = list(range(1, group))
    steps = near + [s * group + i for i in range(group) for s in far]
    order = [0] + far

    barrier = pltpu.get_barrier_semaphore()
    for s in steps:
        pl.semaphore_signal(barrier, inc=1, device_id=(flipped(me, s, n), patch), device_id_type=MESH)
    for p in (up, down):
        pl.semaphore_signal(barrier, inc=1, device_id=(me, p), device_id_type=MESH)
    load_obs = pltpu.make_async_copy(obs_hbm, obs_s, loc.at[6])
    load_obs.start()
    own_obs = pltpu.make_async_copy(obs_hbm.at[:, cols(me, own)], obs_v.at[cols(me, rows), :], loc.at[0])
    own_obs.start()
    small = [
        pltpu.make_async_copy(src, dst, loc.at[3 + i])
        for i, (src, dst) in enumerate(((val_hbm, val_v), (wgt_hbm, wgt_v), (cnt_hbm, cnt_s)))
    ]
    for c in small:
        c.start()
    load_state = pltpu.make_async_copy(state_hbm, state_s, loc.at[7])
    load_state.start()
    own_state = pltpu.make_async_copy(state_hbm.at[:, cols(me, width)], state_v.at[cols(me, rows), :], loc.at[1])
    own_state.start()

    def obs_copy(s):
        peer = flipped(me, s, n)
        return pltpu.make_async_remote_copy(
            src_ref=obs_s.at[:, cols(peer, own)], dst_ref=obs_v.at[cols(me, rows), :],
            send_sem=obs_ss.at[s], recv_sem=obs_rs.at[s], device_id=(peer, patch), device_id_type=MESH)

    def state_copy(s, c):
        peer = flipped(me, s, n)
        return pltpu.make_async_remote_copy(
            src_ref=state_s.at[:, part(peer, c)], dst_ref=state_v.at[cols(me, rows), pl.ds(c * wc, wc)],
            send_sem=st_ss.at[c, s], recv_sem=st_rs.at[c, s], device_id=(peer, patch), device_id_type=MESH)

    def out_copy(s, c):
        peer = flipped(me, s, n)
        return pltpu.make_async_remote_copy(
            src_ref=out_v.at[cols(peer, rows), pl.ds(c * wc, wc)], dst_ref=out_hbm.at[:, part(me, c)],
            send_sem=out_ss.at[c, s], recv_sem=out_rs.at[c, s], device_id=(peer, patch), device_id_type=MESH)

    def edge_copy(slot, s):
        block = cols(flipped(me, s, n), rows)
        return pltpu.make_async_remote_copy(
            src_ref=obs_v.at[block, pl.ds((1 - slot) * half, half)], dst_ref=edge_v.at[slot, block, :],
            send_sem=edge_ss.at[slot, s], recv_sem=edge_rs.at[slot, s],
            device_id=(me, down if slot else up), device_id_type=MESH)

    def side_copy(slot):
        return pltpu.make_async_remote_copy(
            src_ref=side.at[1 - slot], dst_ref=side.at[2 + slot],
            send_sem=side_ss.at[slot], recv_sem=side_rs.at[slot],
            device_id=(me, down if slot else up), device_id_type=MESH)

    load_obs.wait()
    own_obs.wait()
    pl.semaphore_wait(barrier, n + 1)
    for s in near:
        obs_copy(s).start()
    for slot in range(2):
        edge_copy(slot, 0).start()
    for s in steps:
        if s >= group:
            obs_copy(s).start()
    load_state.wait()
    for c in range(CHUNKS):
        for s in steps:
            state_copy(s, c).start()

    for c in small:
        c.wait()
    count = cnt_s[me]
    roots = []
    for k in range(2):
        lane = lax.broadcasted_iota(jnp.int32, (1, half), 1) + k * half
        mask = jnp.where(lane < count, 1.0, 0.0)
        roots.append(jnp.sqrt(wgt_v[pl.ds(2 * me + k, 1), :] * mask))

    for s in steps:
        obs_copy(s).wait_recv()
        for slot in (1, 0):
            edge_copy(slot, s).start()

    def perturb(k, block, at, centre, root):
        scaled_block = ((block.astype(f32) - centre) * root).astype(bf)
        gain[k, at, :] = scaled_block
        gain_t[pl.ds(k * half, half), at] = scaled_block.T

    innovs = [None] * 4

    def innov(k, centre, root, values):
        innovs[k] = (root * (values - centre)).astype(bf).astype(f32)

    for k in range(2):
        block = obs_v[:, k * half:(k + 1) * half]
        centre = rows_sum(block.astype(f32)) * (1.0 / members)
        values = val_v[pl.ds(2 * me + k, 1), :]
        pick = lax.broadcasted_iota(jnp.int32, (8, half), 0)
        side[k] = jnp.where(pick == 0, roots[k], jnp.where(pick == 1, values, centre))
        innov(k, centre, roots[k], values)
        perturb(k, block, pl.ds(0, members), centre, roots[k])
    for slot in range(2):
        side_copy(slot).start()
    for slot in range(2):
        side_copy(slot).wait_recv()
    edge_root, edge_centre = [], []
    for slot in range(2):
        root, values, centre = (side[2 + slot, pl.ds(i, 1), :] for i in range(3))
        edge_root.append(root)
        edge_centre.append(centre)
        innov(2 + slot, centre, root, values)
    dvec = jnp.concatenate(innovs, axis=1)

    def gains_of(at):
        return jnp.concatenate([gain[k, at, :] for k in range(4)], axis=1)

    def state_waits(c):
        if c == 0:
            own_state.wait()
        for s in steps:
            state_copy(s, c).wait_recv()

    normal = None
    for i, s in enumerate(order):
        base = flipped(me // group, s, groups)
        at = cols(base, gr)
        for slot in range(2):
            for j in range(group):
                edge_copy(slot, s * group + j).wait_recv()
        for slot in range(2):
            perturb(2 + slot, edge_v[slot, at, :], at, edge_centre[slot], edge_root[slot])
        piece = dot(gain_t[:, at], gains_of(at))
        if i < groups - 1:
            acc[...] = piece if i == 0 else acc[...] + piece
        else:
            normal = piece if i == 0 else acc[...] + piece

    state_waits(0)
    upper = jnp.max(jnp.sum(jnp.abs(normal), axis=0, keepdims=True), axis=1, keepdims=True)
    upper = upper * (1.0 / (members - 1)) + 1e-06
    t = normal * (2.0 / (members - 1) / upper)
    d1[pl.ds(0, nobs), :] = t.astype(bf)
    d1[pl.ds(nobs, PAD), :] = pair_rows(dvec)

    gsum = jnp.sum(gain_t[...].astype(f32), axis=1, keepdims=True)

    def product_of(c):
        block = state_v[:, c * wc:(c + 1) * wc]
        csum = rows_sum(block.astype(f32))
        return dot(gain_t[...], block) - gsum * (csum * (1.0 / members))

    product = product_of(0)
    nodes, table = functionals()
    wide = jnp.broadcast_to(upper, (1, nobs))
    f_samples, e_samples = [], []
    for k in range(DEGREE + 1):
        m = wide * float(nodes[k])
        lifted = jnp.sqrt(1.0 + m)
        f_samples.append(-1.0 / (lifted * (1.0 + lifted)))
        e_samples.append(1.0 / (1.0 + m))

    def combined(samples):
        out = []
        for j in range(DEGREE + 1):
            total = samples[0] * float(table[j, 0])
            for k in range(1, DEGREE + 1):
                total = total + samples[k] * float(table[j, k])
            out.append(total)
        return out

    fa = combined(f_samples)
    ea = combined(e_samples)
    top, extra = pl.ds(0, nobs), pl.ds(nobs, PAD)
    scale = 1.0 / (members - 1)
    fc = [coef[:, :1] for coef in fa]

    r1 = d1[top, :]
    p0 = product.astype(bf)
    squared = dot(d1[...], r1)
    tp = dot(r1, p0)
    second = 2.0 * squared[:nobs] - 4.0 * t
    y1 = rows_sum(squared[nobs:])
    d2[top, :] = second.astype(bf)
    d2[extra, :] = pair_rows(y1, dvec)
    r2 = d2[top, :]
    tp0 = tp.astype(bf)
    fourth = dot(d2[...], r2)
    sp = dot(r2, p0)
    stp = dot(r2, tp0)
    y2 = fourth[nobs + 2:nobs + 3]
    y3 = 2.0 * (fourth[nobs:nobs + 1] + fourth[nobs + 1:nobs + 2]) + y1 - 2.0 * y2
    d4[...] = (2.0 * fourth[:nobs] + 4.0 * second).astype(bf)
    last = pair_rows(ea[4] * dvec + ea[5] * y1 + ea[6] * y2 + ea[7] * y3)
    tail = rows_sum(dot(last, d4[...]))
    u = pair_rows(ea[0] * dvec + ea[1] * y1 + ea[2] * y2 + ea[3] * y3 + tail)

    def finish(product, tp, sp, stp, c):
        here = pl.ds(c * wc, wc)
        thirdp = 2.0 * stp + tp - 2.0 * sp
        q = fc[4] * product + fc[5] * tp + fc[6] * sp + fc[7] * thirdp
        low = fc[0] * product + fc[1] * tp + fc[2] * sp + fc[3] * thirdp
        mix[...] = ((low + dot(d4[...], q.astype(bf))) * scale).astype(bf)
        shift = rows_sum(dot(u, product.astype(bf))) * scale
        for s in far + [0]:
            base = flipped(mine, s, groups)
            at = cols(base, gr)
            update = dot(gains_of(at), mix[...])
            out_v[at, here] = (state_v[at, here].astype(f32) + shift + update).astype(bf)
            for j in range(group):
                if s * group + j:
                    out_copy(s * group + j, c).start()

    finish(product, tp, sp, stp, 0)
    for c in range(1, CHUNKS):
        state_waits(c)
        product = product_of(c)
        p0 = product.astype(bf)
        tp = dot(d1[top, :], p0)
        finish(product, tp, dot(d2[top, :], p0), dot(d2[top, :], tp.astype(bf)), c)
    keep = pltpu.make_async_copy(out_v.at[cols(me, rows), :], out_hbm.at[:, cols(me, width)], loc.at[2])
    keep.start()

    for slot in range(2):
        side_copy(slot).wait_send()
        for s in range(n):
            edge_copy(slot, s).wait_send()
    for s in steps:
        obs_copy(s).wait_send()
        for c in range(CHUNKS):
            state_copy(s, c).wait_send()
    keep.wait()
    for c in range(CHUNKS):
        for s in steps:
            out_copy(s, c).wait()


def on_device(n, npatch, state, obs_ens, obs_values, obs_weight, counts):
    rows = obs_ens.shape[0]
    own = obs_ens.shape[1] // n
    width = state.shape[1] // n
    members = rows * n
    nobs = 2 * own
    half = own // 2
    wc = width // CHUNKS
    bf, f32 = jnp.bfloat16, jnp.float32
    dma = pltpu.SemaphoreType.DMA
    hbm = pl.BlockSpec(memory_space=pl.ANY)
    return pl.pallas_call(
        functools.partial(kernel, n, npatch),
        out_shape=jax.ShapeDtypeStruct(state.shape, bf),
        in_specs=[pl.BlockSpec(memory_space=pltpu.HBM)] * 5,
        out_specs=hbm,
        scratch_shapes=[
            pltpu.VMEM((2 * n, half), f32),
            pltpu.VMEM((2 * n, half), f32),
            pltpu.SMEM((n,), jnp.int32),
            pltpu.VMEM((4, 8, half), f32),
            pltpu.VMEM(obs_ens.shape, bf),
            pltpu.VMEM(state.shape, bf),
            pltpu.VMEM((2, members, half), bf),
            pltpu.VMEM((members, own), bf),
            pltpu.VMEM((members, width), bf),
            pltpu.VMEM((4, members, half), bf),
            pltpu.VMEM((nobs, members), bf),
            pltpu.VMEM((nobs, nobs), f32),
            pltpu.VMEM((members, width), bf),
            pltpu.VMEM((nobs + PAD, nobs), bf),
            pltpu.VMEM((nobs + PAD, nobs), bf),
            pltpu.VMEM((nobs, nobs), bf),
            pltpu.VMEM((nobs, wc), bf),
            dma((n,)), dma((n,)), dma((CHUNKS, n)), dma((CHUNKS, n)),
            dma((2, n)), dma((2, n)), dma((2,)), dma((2,)), dma((CHUNKS, n)), dma((CHUNKS, n)), dma((8,)),
        ],
        compiler_params=pltpu.CompilerParams(collective_id=0, has_side_effects=True, vmem_limit_bytes=28 * 1024 * 1024),
    )(*(pltpu.with_memory_space_constraint(x, pltpu.HBM) for x in (obs_values.reshape(2 * n, half), obs_weight.reshape(2 * n, half), counts, obs_ens, state)))


def solution(mesh):
    placed = (P("mem", "patch"), P("mem", "patch"), P("patch"), P("patch"), P("patch"))
    body = functools.partial(on_device, mesh.shape["mem"], mesh.shape["patch"])
    return jax.shard_map(
        body, mesh=mesh, in_specs=placed, out_specs=P("mem", "patch"), check_vma=False
    )
```
